8 devices in a mesh: dp: 1 (over z), tp: 2 (over y), cp: 4 (over x, core).
Axes of the slice: x: 2, y: 2, z: 1, core: 2. Of those that a mesh axis runs over, the one named last changes fastest.
Arguments:
- tokens: bfloat16 [2048, 5120], P(('dp', 'tp', 'cp'))
- norm_attn: bfloat16 [2, 5120], replicated
- norm_mlp: bfloat16 [2, 5120], replicated
- w_q: bfloat16 [2, 5120, 32, 128], P(None, None, 'tp')
- w_k: bfloat16 [2, 5120, 1024], P(None, None, 'tp')
- w_v: bfloat16 [2, 5120, 1024], P(None, None, 'tp')
- w_o: bfloat16 [2, 32, 128, 5120], P(None, 'tp')
- w_gate: bfloat16 [2, 5120, 14336], P(None, None, 'tp')
- w_up: bfloat16 [2, 5120, 14336], P(None, None, 'tp')
- w_down: bfloat16 [2, 14336, 5120], P(None, 'tp')
Outputs:
- output: bfloat16 [2048, 5120], P(('dp', 'tp', 'cp'))
All inputs are finite; a program needn't handle non-finite values.
Results may differ from the reference program's by a relative error of at most 0.0167808.
Values are sent between devices in bfloat16 or wider.
A program may use at most 2.25 GiB of HBM per device.

```python
import math
import jax
import jax.numpy as jnp
from jax import lax

D = 5120
FF = 14336
HEADS = 32
KV_HEADS = 8
HEAD = 128
SEQ = 2048
SEGMENT = 128
LAYERS = 2

GROUP = HEADS // KV_HEADS
GROUP_DEVICES = SEQ // (2 * SEGMENT)


def row_positions():
    row_idx = jnp.arange(SEQ)
    device_idx = row_idx // (2 * SEGMENT)
    offset = row_idx % (2 * SEGMENT)
    seg_idx = jnp.where(offset < SEGMENT, device_idx, 2 * GROUP_DEVICES - 1 - device_idx)
    return seg_idx * SEGMENT + offset % SEGMENT


def rms_norm(hidden, gain):
    hidden_f = hidden.astype(jnp.float32)
    inv_rms = lax.rsqrt(jnp.mean(hidden_f * hidden_f, axis=-1, keepdims=True) + 1e-5)
    return (hidden_f * inv_rms * gain.astype(jnp.float32)).astype(jnp.bfloat16)


def rotary(values, positions):
    half_dim = values.shape[-1] // 2
    inv_freq = 500000.0 ** (-(jnp.arange(half_dim, dtype=jnp.float32) * 2.0 / values.shape[-1]))
    angles = positions.astype(jnp.float32)[:, None] * inv_freq[None, :]
    cos_ang = jnp.cos(angles)[:, None, :]
    sin_ang = jnp.sin(angles)[:, None, :]
    first = values[..., :half_dim]
    second = values[..., half_dim:]
    return jnp.concatenate([first * cos_ang - second * sin_ang, second * cos_ang + first * sin_ang], axis=-1)


def attention(queries, keys, value_rows, positions):
    keys_f = keys.astype(jnp.float32)
    values_f = value_rows.astype(jnp.float32)
    q_blocks = queries.reshape(SEQ // SEGMENT, SEGMENT, KV_HEADS, GROUP, HEAD)
    pos_blocks = positions.reshape(SEQ // SEGMENT, SEGMENT)
    scale = 1.0 / math.sqrt(HEAD)

    def one_block(block):
        q_blk, pos_blk = block
        scores = jnp.einsum('bkgd,tkd->bkgt', q_blk.astype(jnp.float32), keys_f) * scale
        visible = positions[None, None, None, :] <= pos_blk[:, None, None, None]
        scores = jnp.where(visible, scores, -jnp.inf)
        row_max = jnp.max(scores, axis=-1, keepdims=True)
        weights = jnp.exp(scores - row_max)
        row_sum = jnp.sum(weights, axis=-1, keepdims=True)
        mixed = jnp.einsum('bkgt,tkd->bkgd', weights.astype(jnp.bfloat16).astype(jnp.float32), values_f)
        return (mixed / row_sum).astype(jnp.bfloat16)

    return lax.map(one_block, (q_blocks, pos_blocks)).reshape(SEQ, HEADS * HEAD)


def layer(hidden, params, positions):
    norm_attn, norm_mlp, w_q, w_k, w_v, w_o, w_gate, w_up, w_down = params
    normed = rms_norm(hidden, norm_attn)
    q_proj = jnp.dot(normed, w_q.reshape(D, HEADS * HEAD), preferred_element_type=jnp.float32)
    queries = rotary(q_proj.reshape(SEQ, HEADS, HEAD), positions).astype(jnp.bfloat16)
    k_proj = jnp.dot(normed, w_k, preferred_element_type=jnp.float32)
    keys = rotary(k_proj.reshape(SEQ, KV_HEADS, HEAD), positions).astype(jnp.bfloat16)
    value_rows = jnp.dot(normed, w_v, preferred_element_type=jnp.float32).astype(jnp.bfloat16).reshape(SEQ, KV_HEADS, HEAD)
    mixed = attention(queries.reshape(SEQ, KV_HEADS, GROUP, HEAD), keys, value_rows, positions)
    attn_out = jnp.dot(mixed, w_o.reshape(HEADS * HEAD, D), preferred_element_type=jnp.float32)
    hidden_mid = (hidden.astype(jnp.float32) + attn_out).astype(jnp.bfloat16)
    normed_mlp = rms_norm(hidden_mid, norm_mlp)
    gate_pre = jnp.dot(normed_mlp, w_gate, preferred_element_type=jnp.float32)
    up_proj = jnp.dot(normed_mlp, w_up, preferred_element_type=jnp.float32)
    hidden_act = (jax.nn.silu(gate_pre) * up_proj).astype(jnp.bfloat16)
    mlp_out = jnp.dot(hidden_act, w_down, preferred_element_type=jnp.float32)
    return (hidden_mid.astype(jnp.float32) + mlp_out).astype(jnp.bfloat16)


def setup_inputs(seed: int = 0, part: int = 0) -> dict:
    key_list = jax.random.split(jax.random.key(seed), 10)
    score_gain = math.sqrt(max(math.log(SEQ) - 2.0, 1.0))
    tokens = jax.random.normal(jax.random.fold_in(key_list[0], part), (SEQ, D), jnp.float32)
    norm_attn = 1.0 + 0.3 * jax.random.normal(key_list[1], (LAYERS, D), jnp.float32)
    norm_mlp = 1.0 + 0.3 * jax.random.normal(key_list[2], (LAYERS, D), jnp.float32)
    w_q = jax.random.normal(key_list[3], (LAYERS, D, HEADS, HEAD), jnp.float32) * (score_gain / math.sqrt(D))
    w_k = jax.random.normal(key_list[4], (LAYERS, D, KV_HEADS * HEAD), jnp.float32) / math.sqrt(D)
    w_v = jax.random.normal(key_list[5], (LAYERS, D, KV_HEADS * HEAD), jnp.float32) / math.sqrt(D)
    w_o = jax.random.normal(key_list[6], (LAYERS, HEADS, HEAD, D), jnp.float32) / math.sqrt(HEADS * HEAD)
    w_gate = jax.random.normal(key_list[7], (LAYERS, D, FF), jnp.float32) / math.sqrt(D)
    w_up = jax.random.normal(key_list[8], (LAYERS, D, FF), jnp.float32) / math.sqrt(D)
    w_down = jax.random.normal(key_list[9], (LAYERS, FF, D), jnp.float32) * (1.5 / math.sqrt(FF))
    return dict(
        tokens=tokens.astype(jnp.bfloat16),
        norm_attn=norm_attn.astype(jnp.bfloat16),
        norm_mlp=norm_mlp.astype(jnp.bfloat16),
        w_q=w_q.astype(jnp.bfloat16),
        w_k=w_k.astype(jnp.bfloat16),
        w_v=w_v.astype(jnp.bfloat16),
        w_o=w_o.astype(jnp.bfloat16),
        w_gate=w_gate.astype(jnp.bfloat16),
        w_up=w_up.astype(jnp.bfloat16),
        w_down=w_down.astype(jnp.bfloat16),
    )


def reference(tokens, norm_attn, norm_mlp, w_q, w_k, w_v, w_o, w_gate, w_up, w_down):
    positions = row_positions()

    def layer_step(hidden, params):
        return layer(hidden, params, positions), None

    stacked = (norm_attn, norm_mlp, w_q, w_k, w_v, w_o, w_gate, w_up, w_down)
    return lax.scan(layer_step, tokens, stacked)[0]
```

```python
import functools
import math
import jax
import jax.numpy as jnp
from jax import lax
from jax.experimental import pallas as pl
from jax.experimental.pallas import tpu as pltpu
from jax.sharding import PartitionSpec as P

F32 = jnp.float32
BF16 = jnp.bfloat16
VMEM_LIMIT = 56 * 1024 * 1024


def rms_norm(hidden, gain):
    hidden_f = hidden.astype(F32)
    inv_rms = lax.rsqrt(jnp.mean(hidden_f * hidden_f, axis=-1, keepdims=True) + 1e-5)
    return (hidden_f * inv_rms * gain.astype(F32)).astype(BF16)


def resident(shape):
    return pl.BlockSpec(shape, lambda j: (0,) * len(shape), pipeline_mode=pl.Buffered(1))


def gate_up_kernel(a_ref, b_ref, wg_ref, wu_ref, o_ref, x_ref):
    seg = a_ref.shape[0]

    @pl.when(pl.program_id(0) == 0)
    def _():
        x_ref[:seg] = a_ref[...]
        x_ref[seg:] = b_ref[...]

    gate = jnp.dot(x_ref[...], wg_ref[...], preferred_element_type=F32)
    up = jnp.dot(x_ref[...], wu_ref[...], preferred_element_type=F32)
    o_ref[...] = (jax.nn.silu(gate) * up).astype(BF16)


def gate_up(own, peer, w_gate, w_up, li, tile=512):
    seg, d = own.shape
    n = w_gate.shape[2]
    wspec = pl.BlockSpec((None, d, tile), lambda j: (li, 0, j))
    return pl.pallas_call(
        gate_up_kernel,
        out_shape=jax.ShapeDtypeStruct((2 * seg, n), BF16),
        grid=(n // tile,),
        in_specs=[resident((seg, d)), resident((seg, d)), wspec, wspec],
        out_specs=pl.BlockSpec((2 * seg, tile), lambda j: (0, j)),
        scratch_shapes=[pltpu.VMEM((2 * seg, d), BF16)],
        compiler_params=pltpu.CompilerParams(vmem_limit_bytes=VMEM_LIMIT),
        cost_estimate=pl.CostEstimate(flops=8 * seg * d * n, bytes_accessed=4 * d * n, transcendentals=2 * seg * n),
    )(own, peer, w_gate, w_up)


def split_kernel(x_ref, w_ref, own_ref, send_ref):
    seg = own_ref.shape[0]
    part = jnp.dot(x_ref[...], w_ref[...], preferred_element_type=F32)
    own_ref[...] = part[:seg]
    send_ref[...] = part[seg:]


def split_proj(x, w, li, tile=512, first=0, count=None):
    rows, k = x.shape
    seg = rows // 2
    n = w.shape[2] if count is None else count
    base = first // tile
    return pl.pallas_call(
        split_kernel,
        out_shape=[jax.ShapeDtypeStruct((seg, n), F32)] * 2,
        grid=(n // tile,),
        in_specs=[resident((rows, k)), pl.BlockSpec((None, k, tile), lambda j: (li, 0, base + j))],
        out_specs=[pl.BlockSpec((seg, tile), lambda j: (0, j))] * 2,
        compiler_params=pltpu.CompilerParams(vmem_limit_bytes=VMEM_LIMIT),
        cost_estimate=pl.CostEstimate(flops=2 * rows * k * n, bytes_accessed=2 * k * n + 4 * rows * n, transcendentals=0),
    )(x, w)


def rotate(x, cos, sin):
    return x * cos + pltpu.roll(x, x.shape[1] // 2, axis=1) * sin


def kv_kernel(a_ref, b_ref, wk_ref, wv_ref, cos_ref, sin_ref, o_ref, x_ref):
    seg = a_ref.shape[0]
    head = cos_ref.shape[1]
    tile = wk_ref.shape[1]
    step = pl.program_id(0)
    width = o_ref.shape[1] // 2

    @pl.when(step == 0)
    def _():
        x_ref[:seg] = a_ref[...]
        x_ref[seg:] = b_ref[...]

    x = x_ref[...]
    k = jnp.dot(x, wk_ref[...], preferred_element_type=F32)
    base = pl.multiple_of(step * tile, tile)
    rot = [rotate(k[:, h:h + head], cos_ref[...], sin_ref[...]).astype(BF16) for h in range(0, tile, head)]
    o_ref[:, pl.ds(base, tile)] = jnp.concatenate(rot, axis=1)
    o_ref[:, pl.ds(width + base, tile)] = jnp.dot(x, wv_ref[...], preferred_element_type=F32).astype(BF16)


def kv_proj(own, peer, w_k, w_v, cos, sin, li, tile=256):
    seg, d = own.shape
    n = w_k.shape[2]
    head = cos.shape[1]
    wspec = pl.BlockSpec((None, d, tile), lambda j: (li, 0, j))
    return pl.pallas_call(
        kv_kernel,
        out_shape=jax.ShapeDtypeStruct((2 * seg, 2 * n), BF16),
        grid=(n // tile,),
        in_specs=[resident((seg, d)), resident((seg, d)), wspec, wspec, resident((2 * seg, head)), resident((2 * seg, head))],
        out_specs=pl.BlockSpec((2 * seg, 2 * n), lambda j: (0, 0)),
        scratch_shapes=[pltpu.VMEM((2 * seg, d), BF16)],
        compiler_params=pltpu.CompilerParams(vmem_limit_bytes=VMEM_LIMIT),
        cost_estimate=pl.CostEstimate(flops=8 * seg * d * n, bytes_accessed=4 * d * n, transcendentals=0),
    )(own, peer, w_k, w_v, cos, sin)


def attn_kernel(seg_q_ref, seg_k_ref, q_ref, cos_ref, sin_ref, *rest, seg, group, head_dim, free, parts):
    total = free + parts
    k_refs = rest[0:2 * total:2]
    v_refs = rest[1:2 * total:2]
    o_ref, s_ref, qs_ref, m_ref, l_ref, acc_ref = rest[2 * total:]
    rate = math.log2(math.e) / math.sqrt(head_dim)
    n_q = q_ref.shape[0] // seg
    rows = group * seg
    q_row = lax.broadcasted_iota(jnp.int32, (seg, seg), 0)
    k_col = lax.broadcasted_iota(jnp.int32, (seg, seg), 1)

    def scores(i, p):
        return lax.dot_general(qs_ref[i], k_refs[p][...], (((1,), (1,)), ((), ())), preferred_element_type=F32)

    def weigh(i, p):
        top = m_ref[i]
        w0 = jnp.exp2((s_ref[i, p, :, :seg] - top) * rate)
        w1 = jnp.exp2((s_ref[i, p, :, seg:] - top) * rate)
        w = jnp.concatenate([w0.astype(BF16), w1.astype(BF16)], axis=1)
        return w0 + w1, jnp.dot(w, v_refs[p][...], preferred_element_type=F32)

    for i in range(n_q):
        cos = cos_ref[i * seg:(i + 1) * seg]
        sin = sin_ref[i * seg:(i + 1) * seg]
        for g in range(group):
            q = q_ref[i * seg:(i + 1) * seg, g * head_dim:(g + 1) * head_dim]
            qs_ref[i, g * seg:(g + 1) * seg, :] = rotate(q, cos, sin).astype(BF16)
        top = jnp.full((rows, seg), -jnp.inf, F32)
        for p in range(free):
            s = scores(i, p)
            s_ref[i, p] = s
            top = jnp.maximum(top, jnp.maximum(s[:, :seg], s[:, seg:]))
        m_ref[i] = top
    seen = {}
    for i in range(n_q):
        sq = seg_q_ref[i]
        for p in range(free, total):
            sk0 = seg_k_ref[2 * (p - free)]
            sk1 = seg_k_ref[2 * (p - free) + 1]
            seen[i, p] = jnp.minimum(sk0, sk1) <= sq

            @pl.when(seen[i, p])
            def _(i=i, p=p, sk0=sk0, sk1=sk1, sq=sq):
                s = scores(i, p)
                top = m_ref[i]
                for b, sk in enumerate((sk0, sk1)):
                    bias = jnp.where(k_col <= q_row + (sq - sk) * seg, 0.0, -jnp.inf)
                    sb = s[:, b * seg:(b + 1) * seg] + jnp.concatenate([bias] * group, axis=0)
                    s_ref[i, p, :, b * seg:(b + 1) * seg] = sb
                    top = jnp.maximum(top, sb)
                m_ref[i] = top

    for i in range(n_q):
        m_ref[i] = jnp.broadcast_to(jnp.max(m_ref[i], axis=-1, keepdims=True), (rows, seg))
        lsum = jnp.zeros((rows, seg), F32)
        acc = jnp.zeros((rows, head_dim), F32)
        for p in range(free):
            wl, wa = weigh(i, p)
            lsum = lsum + wl
            acc = acc + wa
        l_ref[i] = lsum
        acc_ref[i] = acc
    for i in range(n_q):
        for p in range(free, total):
            @pl.when(seen[i, p])
            def _(i=i, p=p):
                wl, wa = weigh(i, p)
                l_ref[i] += wl
                acc_ref[i] += wa

    for i in range(n_q):
        out = acc_ref[i] / jnp.sum(l_ref[i], axis=-1, keepdims=True)
        for g in range(group):
            o_ref[i * seg:(i + 1) * seg, g * head_dim:(g + 1) * head_dim] = out[g * seg:(g + 1) * seg, :].astype(BF16)


def attend(q_raw, cos, sin, free_parts, kv_parts, seg_q, seg_k, seg, group, head_dim):
    rows = q_raw.shape[0]
    n_q = rows // seg
    width = group * head_dim
    kv_loc = q_raw.shape[1] // width
    every = list(free_parts) + list(kv_parts)
    total = len(every)
    k_spec = pl.BlockSpec((2 * seg, head_dim), lambda h, *_: (0, h))
    v_spec = pl.BlockSpec((2 * seg, head_dim), lambda h, *_: (0, kv_loc + h))
    t_spec = pl.BlockSpec((rows, head_dim), lambda h, *_: (0, 0))
    q_spec = pl.BlockSpec((rows, width), lambda h, *_: (0, h))
    keys = total * 2 * seg
    return pl.pallas_call(
        functools.partial(attn_kernel, seg=seg, group=group, head_dim=head_dim, free=len(free_parts), parts=len(kv_parts)),
        out_shape=jax.ShapeDtypeStruct((rows, kv_loc * width), BF16),
        grid_spec=pltpu.PrefetchScalarGridSpec(
            num_scalar_prefetch=2,
            grid=(kv_loc,),
            in_specs=[q_spec, t_spec, t_spec] + [k_spec, v_spec] * total,
            out_specs=q_spec,
            scratch_shapes=[
                pltpu.VMEM((n_q, total, group * seg, 2 * seg), F32),
                pltpu.VMEM((n_q, group * seg, head_dim), BF16),
                pltpu.VMEM((n_q, group * seg, seg), F32),
                pltpu.VMEM((n_q, group * seg, seg), F32),
                pltpu.VMEM((n_q, group * seg, head_dim), F32),
            ],
        ),
        compiler_params=pltpu.CompilerParams(vmem_limit_bytes=32 * 1024 * 1024),
        cost_estimate=pl.CostEstimate(
            flops=4 * rows * keys * kv_loc * width,
            bytes_accessed=rows * kv_loc * width * 6 + keys * kv_loc * head_dim * 4,
            transcendentals=rows * keys * kv_loc * group,
        ),
    )(seg_q, seg_k, q_raw, cos, sin, *[v for part in every for v in (part, part)])


def solution(mesh):
    tp_size = mesh.shape['tp']
    cp_size = mesh.shape['cp']
    dev_total = tp_size * cp_size
    row_spec = P(('dp', 'tp', 'cp'), None)
    gain_spec = P(None, None)
    q_spec = P(None, None, 'tp', None)
    col_spec = P(None, None, 'tp')
    o_spec = P(None, 'tp', None, None)
    down_spec = P(None, 'tp', None)
    swap = [(0, 1), (1, 0)]

    def body(tokens, norm_attn, norm_mlp, w_q, w_k, w_v, w_o, w_gate, w_up, w_down):
        layers = w_q.shape[0]
        d_model = tokens.shape[1]
        heads_loc = w_q.shape[2]
        head_dim = w_q.shape[3]
        kv_cols = w_k.shape[2]
        kv_loc = kv_cols // head_dim
        group = heads_loc // kv_loc
        half = head_dim // 2
        seg = tokens.shape[0] // 2
        tp_idx = lax.axis_index('tp')
        cp_idx = lax.axis_index('cp')
        tps = jnp.stack([tp_idx, 1 - tp_idx])
        cps = jnp.stack([cp_idx, cp_idx ^ 1, cp_idx ^ 2, cp_idx ^ 3])
        dev_q = tps * cp_size + cp_idx
        dev_k = jnp.stack([tps * cp_size + cps[0], tps * cp_size + cps[1], tps * cp_size + cps[2], tps * cp_size + cps[3]]).reshape(-1)
        seg_q = [dev_q, 2 * dev_total - 1 - dev_q]
        seg_k = [dev_k, 2 * dev_total - 1 - dev_k]
        inv_freq = 500000.0 ** (-(jnp.arange(half, dtype=F32) * 2.0 / head_dim))
        cos, sin = [], []
        for c in range(2):
            pos = (seg_q[c][:, None] * seg + jnp.arange(seg)[None, :]).reshape(-1)
            ang = pos.astype(F32)[:, None] * inv_freq[None, :]
            c_half, s_half = jnp.cos(ang), jnp.sin(ang)
            cos.append(jnp.concatenate([c_half, c_half], axis=1))
            sin.append(jnp.concatenate([-s_half, s_half], axis=1))

        def swap_tp(v):
            return lax.ppermute(v, 'tp', swap)

        def swap_cp(v, bit):
            return lax.ppermute(v, 'cp', [(i, i ^ bit) for i in range(cp_size)])

        def after(v, *tokens_):
            return lax.optimization_barrier((v,) + tokens_)[0]

        def gather_kv(kv):
            core = swap_cp(kv, 1)
            cross = swap_cp(kv, 2)
            return [kv, core, cross, swap_cp(cross, 1)]

        def kv_of(own, peer, li, c):
            return kv_proj(own, peer, w_k, w_v, cos[c], sin[c], li)

        def q_of(own, peer, wq):
            nn = jnp.concatenate([own, peer], axis=0)
            return jnp.einsum('rd,dhe->rhe', nn, wq, preferred_element_type=F32).reshape(2 * seg, heads_loc * head_dim)

        def mix_a(q, parts):
            return attend(q, cos[0], sin[0], [], parts, seg_q[0], seg_k[0], seg, group, head_dim)

        def mix_b(q, parts_a, parts_b):
            return attend(q, cos[1], sin[1], parts_a, parts_b, seg_q[1], seg_k[1], seg, group, head_dim)

        def add(base, part, other):
            return (base.astype(F32) + (part + other)).astype(BF16)

        wo = w_o.reshape(layers, heads_loc * head_dim, d_model)
        xa, xb = tokens[:seg], tokens[seg:]
        na = rms_norm(xa, norm_attn[0])
        nb = rms_norm(xb, norm_attn[0])
        nap, nbp = swap_tp(na), swap_tp(nb)
        wq = after(w_q, na, nb)[0]
        for li in range(layers):
            kva = kv_of(na if li else after(na, wq), nap, li, 0)
            parts_a = gather_kv(kva)
            qa = q_of(na, after(nap, kva), wq)
            if li > 0:
                ma = mix_a(qa, parts_a)
                pa, sa = split_proj(ma, wo, li, 2560)
                xb = add(hb, down_b, after(rb, pa))
                nb = rms_norm(xb, norm_attn[li])
                nbp = swap_tp(nb)
                ra = swap_tp(after(sa, nb))
                kvb = kv_of(nb, nbp, li, 1)
                parts_b = gather_kv(kvb)
                qb = q_of(nb, after(nbp, kvb), wq)
            else:
                kvb = kv_of(after(nb, qa), nbp, li, 1)
                parts_b = gather_kv(kvb)
                qb = q_of(nb, after(nbp, kvb), wq)
                ma = mix_a(after(qa, qb), parts_a)
                pa, sa = split_proj(ma, wo, li, 2560)
                ra = swap_tp(sa)
            mb = mix_b(after(qb, pa), parts_a, parts_b)
            pb, sb = split_proj(mb, wo, li, 2560)
            ha = add(xa, pa, after(ra, pb))
            na = rms_norm(ha, norm_mlp[li])
            nap = swap_tp(na)
            rb = swap_tp(after(sb, na))
            if li + 1 < layers:
                wq = after(w_q, na)[li + 1]
                na = after(na, wq)
            act_a = gate_up(na, nap, w_gate, w_up, li)
            hb = add(xb, pb, after(rb, act_a))
            nb = rms_norm(hb, norm_mlp[li])
            nbp = swap_tp(nb)
            down_a, sa = split_proj(after(act_a, nb), w_down, li)
            ra = swap_tp(sa)
            act_b = gate_up(after(nb, down_a), nbp, w_gate, w_up, li)
            xa = add(ha, down_a, after(ra, act_b))
            if li + 1 < layers:
                na = rms_norm(xa, norm_attn[li + 1])
                nap = swap_tp(na)
            down_b, sb = split_proj(after(act_b, xa), w_down, li)
            rb = swap_tp(sb)
        xb = add(hb, down_b, rb)
        return jnp.concatenate([xa, xb], axis=0)

    return jax.shard_map(
        body,
        mesh=mesh,
        in_specs=(row_spec, gain_spec, gain_spec, q_spec, col_spec, col_spec, o_spec, col_spec, col_spec, down_spec),
        out_specs=row_spec,
        check_vma=False,
    )
```
